32 devices in a mesh: gx: 4 (over y, core), gy: 2 (over x), gz: 4 (over z).
Axes of the slice: x: 2, y: 2, z: 4, core: 2. Of those that a mesh axis runs over, the one named last changes fastest.
Arguments:
- pressure_now: float32 [64, 64, 512], P('gx', 'gy', 'gz'), may hold values from -6 to 6
- pressure_before: float32 [64, 64, 512], P('gx', 'gy', 'gz'), may hold values from -6 to 6
- region_code: int32 [64, 64, 512], P('gx', 'gy', 'gz'), may hold values from 0 to 7
- velocity: float32 [8], replicated, may hold values from 0.2 to 0.42
- wavelet: float32 [6, 16], replicated, may hold values from -6 to 6
- source_cell: int32 [16], replicated, may hold values from 0 to 2097151
Outputs:
- pressure: float32 [64, 64, 512], P('gx', 'gy', 'gz')
- previous: float32 [64, 64, 512], P('gx', 'gy', 'gz')
The draws below stay inside these ranges and needn't reach their ends.
Inputs may be any that keep to these rules, and one draw needn't show every extreme that they name: source_cell[s] is the flat index x * 64 * 512 + y * 512 + z of a grid cell; sources may share a cell.
All inputs are finite; a program needn't handle non-finite values.
Results may differ from the reference program's by a relative error of at most 0.00002.
Values sent between devices are 32-bit elements; how exact they have to be, the bound alone decides.
A program may use at most 64 MiB of HBM per device.

```python
import math
import jax
import jax.numpy as jnp
from jax import lax

STEPS = 6
NSRC = 16
NREG = 8
NX = 64
NY = 64
NZ = 512


def touch_ends(array, rng, least, top_value):
    extent = array.shape
    place = [jax.random.randint(jax.random.fold_in(rng, axis), (), 0, extent[axis]) for axis in range(len(extent))]
    array = array.at[tuple(place)].set(least)
    longest = extent.index(max(extent))
    place[longest] = (place[longest] + 1) % extent[longest]
    return array.at[tuple(place)].set(top_value)


def steps_of(rng, dims, cuts, low, largest):
    factor_of, own = 1.0, jax.random.fold_in(rng, 6)
    for position, blocks in cuts:
        steps = jnp.exp(jax.random.uniform(jax.random.fold_in(own, position), (blocks,), jnp.float32, low / len(cuts), largest / len(cuts)))
        factor_of = factor_of * jnp.repeat(steps, dims[position] // blocks).reshape([-1 if axis == position else 1 for axis in range(len(dims))])
    return factor_of


def noise(own_key, extent, spread, limit, split=(), dtype=jnp.bfloat16):
    level = steps_of(own_key, extent, split, -0.22, 0.18) if split else 1.0
    result = jax.random.normal(own_key, extent, jnp.float32) * spread * level
    return jnp.minimum(jnp.maximum(result, -limit), limit).astype(dtype)


def setup_inputs(seed: int = 0) -> dict:
    splits = jax.random.split(jax.random.key(seed), 7)
    return {
        "pressure_now": noise(splits[0], (NX, NY, NZ), 1.0, 6.0, ((0, 4), (1, 2), (2, 4)), jnp.float32),
        "pressure_before": noise(splits[1], (NX, NY, NZ), 1.0, 6.0, ((0, 4), (1, 2), (2, 4)), jnp.float32),
        "region_code": touch_ends(jax.random.randint(splits[2], (NX, NY, NZ), 0, NREG), jax.random.fold_in(splits[2], 1), 0, NREG - 1).astype(jnp.int32),
        "velocity": jnp.clip(jnp.exp(jax.random.uniform(splits[3], (NREG,), jnp.float32, math.log(0.2), math.log(0.42))), 0.2, 0.42),
        "wavelet": noise(splits[4], (STEPS, NSRC), 1.0, 6.0, (), jnp.float32),
        "source_cell": touch_ends(jax.random.randint(splits[5], (NSRC,), 0, NX * NY * NZ), jax.random.fold_in(splits[5], 1), 0, (NX * NY * NZ) - 1).astype(jnp.int32),
    }


CENTRE = -205.0 / 72.0
WEIGHTS = (8.0 / 5.0, -1.0 / 5.0, 8.0 / 315.0, -1.0 / 560.0)


def cut(field, start, size):
    return lax.slice(field, tuple(start), tuple(a + b for a, b in zip(start, size)))


def along(field, axis, start, size):
    total = None
    for step_k, weight in enumerate(WEIGHTS, 1):
        upper = list(start)
        upper[axis] = upper[axis] + step_k
        lower = list(start)
        lower[axis] = lower[axis] - step_k
        term = weight * (cut(field, upper, size) + cut(field, lower, size))
        total = term if total is None else total + term
    return total


def reference(pressure_now, pressure_before, region_code, velocity, wavelet, source_cell):
    size = pressure_now.shape
    speed = velocity[region_code]
    rate = speed * speed
    current = pressure_now
    before = pressure_before
    for step in range(STEPS):
        padded = jnp.pad(current, ((4, 4), (0, 0), (0, 0)), mode="wrap")
        padded = jnp.pad(padded, ((0, 0), (4, 4), (4, 4)))
        start = (4, 4, 4)
        laplace = 3.0 * CENTRE * current + along(padded, 0, start, size) + along(padded, 1, start, size) + along(padded, 2, start, size)
        following = 2.0 * current - before + rate * laplace
        following = following.reshape(-1).at[source_cell].add(wavelet[step]).reshape(size)
        before = current
        current = following
    return current, before
```

```python
import functools

import jax
import jax.numpy as jnp
from jax import lax
from jax.experimental import pallas as pl
from jax.experimental.pallas import tpu as pltpu
from jax.sharding import PartitionSpec as P

STEPS = 6
CENTRE = -205.0 / 72.0
C1, C2, C3, C4 = (8.0 / 5.0, -1.0 / 5.0, 8.0 / 315.0, -1.0 / 560.0)
SCALE = 5040.0
WEIGHTS = tuple(round(SCALE * c) * 1.0 for c in (C1, C2, C3, C4))
W = 4
CHUNKS = 1
T = 8
LANES = 128
MESH = pl.DeviceIdType.MESH
def kernel(sizes, now_hbm, before_hbm, code_hbm, vel_ref, wave_ref, src_ref, out_ref, prev_ref,
           field0, field1, beside0, beside1, state0, state1, pack0, pack1, halo, rate, coef, code, source, edge,
           along, along_z, from_edge, only, send_sem, recv_sem, load_sem):
    field, beside, state, pack = (field0, field1), (beside0, beside1), (state0, state1), (pack0, pack1)
    (nx, ny, nz), (gx, gy, gz) = sizes
    grid_y, grid_z = ny * gy, nz * gz
    lanes_of = ny // 8
    slabs = LANES // 8 // lanes_of
    packs = nx // slabs
    ix, iy, iz = lax.axis_index("gx"), lax.axis_index("gy"), lax.axis_index("gz")
    targets = (
        (({"gx": lax.rem(ix + gx - 1, gx)}, None), ({"gx": lax.rem(ix + 1, gx)}, None)),
        (({"gy": iy - 1}, iy > 0), ({"gy": iy + 1}, iy < gy - 1)),
        (({"gz": iz - 1}, iz > 0), ({"gz": iz + 1}, iz < gz - 1)),
    )

    def guarded(condition, action):
        if condition is None:
            action()
        else:
            pl.when(condition)(action)

    own_x, own_y = pl.ds(0, nx), pl.ds(T, ny)
    half = lanes_of // CHUNKS
    loads = [
        pltpu.make_async_copy(now_hbm, field[0].at[own_x, own_y], load_sem.at[0]),
        pltpu.make_async_copy(before_hbm, field[1].at[own_x, own_y], load_sem.at[1]),
        pltpu.make_async_copy(code_hbm, code, load_sem.at[2]),
    ]
    for load in loads:
        load.start()

    nothing = jnp.zeros((nx, T, LANES), jnp.float32)
    for par in range(2):
        field[par][own_x, 0:T, :] = nothing
        field[par][own_x, pl.ds(T + ny, T), :] = nothing
        beside[par][...] = jnp.zeros_like(beside[par])
    edge[...] = jnp.zeros_like(edge)

    barrier = pltpu.get_barrier_semaphore()
    for sides in targets:
        for target, present in sides:
            guarded(present, lambda target=target: pl.semaphore_signal(
                barrier, inc=1, device_id=target, device_id_type=MESH))

    inner = packs - 2

    def group(name, par):
        pieces = []
        if name[0] == "x":
            base = 2 * name[1]
            part = pl.ds(name[1] * half, half)
            pieces = [(0, state[par].at[pl.ds(0, W), part], halo.at[par, 1, name[1]]),
                      (0, state[par].at[pl.ds(nx - W, W), part], halo.at[par, 0, name[1]])]
        else:
            axis = 1 if name[0] == "y" else 2
            base = 2 * CHUNKS + (0 if axis == 1 else 6)
            if axis == 1:
                low, high = pl.ds(T, W), pl.ds(T + ny - W, W)
                over, under = pl.ds(T + ny, W), pl.ds(T - W, W)
                if name[1] == "face":
                    spans = [pl.ds(0, slabs), pl.ds(nx - slabs, slabs)]
                else:
                    spans = [pl.ds(slabs, nx - 2 * slabs)]
                    base = base + 4
                for span in spans:
                    pieces.append((1, field[par].at[span, low], beside[par].at[span, over]))
                    pieces.append((1, field[par].at[span, high], beside[par].at[span, under]))
            else:
                span = pl.ds(0, 2) if name[1] == "face" else pl.ds(2, inner)
                base = base + (0 if name[1] == "face" else 2)
                pieces.append((2, pack[par].at[span], edge.at[par, 1, span]))
                pieces.append((2, pack[par].at[span], edge.at[par, 0, span]))
        result = []
        for n, (axis, src, dst) in enumerate(pieces):
            target, present = targets[axis][n % 2]
            copy = pltpu.make_async_remote_copy(
                src_ref=src, dst_ref=dst, send_sem=send_sem.at[par, base + n], recv_sem=recv_sem.at[par, base + n],
                device_id=target, device_id_type=MESH)
            result.append((copy, present, targets[axis][1 - n % 2][1]))
        return result

    def start(name, par):
        for copy, to_here, _ in group(name, par):
            guarded(to_here, copy.start)

    def wait_send(name, par):
        for copy, to_here, _ in group(name, par):
            guarded(to_here, copy.wait_send)

    def wait_recv(name, par):
        for copy, _, from_here in group(name, par):
            guarded(from_here, copy.wait_recv)

    chunks = [("x", n) for n in range(CHUNKS)]
    every = chunks + [("y", "face"), ("z", "face"), ("y", "inner"), ("z", "inner")]

    lane = lax.broadcasted_iota(jnp.int32, (8, LANES), 1)
    group_of, place = lane // 8, lane % 8

    def packed(value, g, total):
        return jnp.where(group_of == g, pltpu.roll(value, (W + 8 * g) % LANES, 1), total)

    def rows(j):
        return pl.ds(T + j, 8, stride=lanes_of)

    zero = jnp.zeros((8, LANES), jnp.float32)
    ends = ((0, 0, 0), (1, 1, nx - slabs))

    loads[0].wait()
    for side, slot, first in ends:
        total = zero
        for a in range(slabs):
            for j in range(lanes_of):
                value = field[0][first + a, rows(j), :]
                state[0][first + a, j] = value
                total = packed(value, a * lanes_of + j, total)
        pack[0][slot] = total
    peers = 2
    for sides in targets[1:]:
        for _, present in sides:
            peers = peers + present.astype(jnp.int32)
    pl.semaphore_wait(barrier, peers)
    for name in chunks + [("y", "face"), ("z", "face"), ("y", "inner")]:
        start(name, 0)

    def first_pack(m, carry):
        total = zero
        for a in range(slabs):
            for j in range(lanes_of):
                value = field[0][m * slabs + slabs + a, rows(j), :]
                state[0][m * slabs + slabs + a, j] = value
                total = packed(value, a * lanes_of + j, total)
        pack[0][2 + m] = total
        return carry

    lax.fori_loop(0, inner, first_pack, 0)
    start(("z", "inner"), 0)

    loads[2].wait()
    squares = [vel_ref[n] * vel_ref[n] for n in range(vel_ref.shape[0])]

    def rate_slab(x, carry):
        for j in range(lanes_of):
            codes = code[x, pl.ds(j, 8, stride=lanes_of), :]
            value = jnp.full(codes.shape, squares[0], jnp.float32)
            for n in range(1, len(squares)):
                value = jnp.where(codes == n, squares[n], value)
            rate[x, j] = value * (1.0 / SCALE)
            coef[x, j] = 2.0 + (3.0 * CENTRE) * value
        return carry

    lax.fori_loop(0, nx, rate_slab, 0)

    count = src_ref.shape[0]
    row_at = jnp.full((1, LANES), -1, jnp.int32)
    lane_row = lax.broadcasted_iota(jnp.int32, (1, LANES), 1)
    slot_col = lax.broadcasted_iota(jnp.int32, (LANES, LANES), 0)
    z_at = jnp.full((LANES, LANES), -1, jnp.int32)
    for s in range(count):
        cell = src_ref[s]
        sx = cell // (grid_y * grid_z) - ix * nx
        sy = cell // grid_z % grid_y - iy * ny
        sz = cell % grid_z - iz * nz
        here = (sx >= 0) & (sx < nx) & (sy >= 0) & (sy < ny)
        local = jnp.where(here, sx * ny + sy % lanes_of * 8 + sy // lanes_of, -1)
        row_at = jnp.where((lane_row % count == s) & (lane_row < 3 * count), local, row_at)
        z_at = jnp.where((slot_col % count == s) & (slot_col < 3 * count), sz, z_at)
    spread = (z_at == lax.broadcasted_iota(jnp.int32, (LANES, LANES), 1)).astype(jnp.float32).astype(jnp.bfloat16)

    def source_field(t):
        wave = jnp.zeros((1, LANES), jnp.float32)
        for s in range(count):
            wave = jnp.where(lane_row % count == s, wave_ref[t, s], wave)
        high = wave.astype(jnp.bfloat16).astype(jnp.float32)
        rest = wave - high
        middle = rest.astype(jnp.bfloat16).astype(jnp.float32)
        parts = jnp.where(lane_row < count, high, jnp.where(lane_row < 2 * count, middle, rest - middle))
        block = slabs * ny

        def chunk(m, carry):
            row = lax.broadcasted_iota(jnp.int32, (block, LANES), 0) + m * block
            picks = jnp.where(row == row_at, parts, 0.0).astype(jnp.bfloat16)
            value = jnp.dot(picks, spread, preferred_element_type=jnp.float32)
            source[pl.ds(m * slabs, slabs)] = value.reshape(slabs, lanes_of, 8, LANES)
            return carry

        lax.fori_loop(0, packs, chunk, 0)

    row_in = lax.broadcasted_iota(jnp.int32, (LANES, LANES), 0)
    col_in = lax.broadcasted_iota(jnp.int32, (LANES, LANES), 1)
    spot = row_in % 8
    halo_at = jnp.where(spot < W, spot - W, LANES + spot - W)

    def taps(distance):
        value = jnp.zeros((LANES, LANES), jnp.float32)
        for k in range(1, W + 1):
            value = jnp.where((distance == k) | (distance == -k), WEIGHTS[k - 1], value)
        return value.astype(jnp.bfloat16)

    for part in range(2):
        along_z[pl.ds(part * LANES, LANES), :] = taps(row_in - col_in)
        from_edge[pl.ds(part * LANES, LANES), :] = taps(halo_at - col_in)
    double_lane = lax.broadcasted_iota(jnp.int32, (16, LANES), 1) // 8
    double_row = lax.broadcasted_iota(jnp.int32, (16, LANES), 0) // 8
    for pair in range(8):
        only[pair] = (double_lane == 2 * pair + double_row).astype(jnp.float32).astype(jnp.bfloat16)

    def split(value):
        high = value.astype(jnp.bfloat16)
        return high, (value - high.astype(jnp.float32)).astype(jnp.bfloat16)

    def z_own(cur):
        value = state[cur][...].reshape(nx * ny, LANES)
        total = jnp.dot(jnp.concatenate(split(value), axis=1), along_z[...], preferred_element_type=jnp.float32)
        along[...] = total.reshape(nx, lanes_of, 8, LANES)

    def z_beside(cur, slots):
        picked = []
        for slot in slots:
            value = jnp.where(place < W, edge[cur, 0, slot], edge[cur, 1, slot])
            high, low = split(jnp.concatenate([value, value], axis=0))
            picked += [jnp.concatenate([high * only[pair], low * only[pair]], axis=1) for pair in range(8)]
        total = jnp.dot(jnp.concatenate(picked, axis=0), from_edge[...], preferred_element_type=jnp.float32)
        return total.reshape(len(slots), slabs, lanes_of, 8, LANES)

    def own_part(cur, nxt, first, ends):
        for a in range(slabs):
            x = first + a
            shifted = {}
            for o in range(-W, lanes_of + W):
                if 0 <= o < lanes_of:
                    shifted[o] = state[cur][x, o]
                else:
                    shifted[o] = field[cur][x, pl.ds(T + o, 8, stride=lanes_of), :]
            for j in range(lanes_of):
                acc = along[x, j]
                for k in range(1, W + 1):
                    near = shifted[j + k] + shifted[j - k]
                    if not ends or x + k < nx:
                        near = near + state[cur][x + k, j]
                    if not ends or x - k >= 0:
                        near = near + state[cur][x - k, j]
                    acc = acc + WEIGHTS[k - 1] * near
                state[nxt][x, j] = (coef[x, j] * shifted[j] - state[nxt][x, j]) + (rate[x, j] * acc + source[x, j])

    def yz_part(cur, nxt, first, beyond):
        results = {}
        for a in range(slabs):
            x = first + a
            outer = {o: beside[cur][x, pl.ds(T + o, 8, stride=lanes_of), :]
                     for o in list(range(-W, 0)) + list(range(lanes_of, lanes_of + W))}
            for j in range(lanes_of):
                acc = beyond[a, j]
                for k in range(1, W + 1):
                    if j - k < 0:
                        acc = acc + WEIGHTS[k - 1] * outer[j - k]
                    if j + k >= lanes_of:
                        acc = acc + WEIGHTS[k - 1] * outer[j + k]
                results[a, j] = state[nxt][x, j] + rate[x, j] * acc
        return results

    def x_part(cur, nxt, x, j, n):
        acc = None
        for k in range(1, W + 1):
            if x - k < 0:
                term = WEIGHTS[k - 1] * halo[cur, 0, n, x - k + W, j - n * half]
            elif x + k >= nx:
                term = WEIGHTS[k - 1] * halo[cur, 1, n, x + k - nx, j - n * half]
            else:
                continue
            acc = term if acc is None else acc + term
        return state[nxt][x, j] + rate[x, j] * acc

    def first_before(x, carry):
        for j in range(lanes_of):
            state[1][x, j] = field[1][x, rows(j), :]
        return carry

    loads[1].wait()
    lax.fori_loop(0, nx, first_before, 0)
    for t in range(STEPS):
        cur, nxt = t % 2, (t + 1) % 2
        last = t == STEPS - 1

        def put(x, j, value):
            own = pl.ds(j, 8, stride=lanes_of)
            if last:
                out_ref[x, own, :] = value
            else:
                state[nxt][x, j] = value
                field[nxt][x, rows(j), :] = value
            if t == STEPS - 2:
                prev_ref[x, own, :] = value

        source_field(t)
        if t >= 1:
            for name in every:
                wait_send(name, nxt)
        z_own(cur)
        for _, _, first in ends:
            own_part(cur, nxt, first, True)
        for m in range(inner):
            own_part(cur, nxt, m * slabs + slabs, False)
        wait_recv(("z", "face"), cur)
        wait_recv(("y", "face"), cur)
        beyond = z_beside(cur, [slot for _, slot, _ in ends])
        for n, (_, slot, first) in enumerate(ends):
            for (a, j), value in yz_part(cur, nxt, first, beyond[n]).items():
                state[nxt][first + a, j] = value
        totals = [zero, zero]
        for n in range(CHUNKS):
            wait_recv(("x", n), cur)
            js = range(n * half, n * half + half)
            for side, slot, first in ends:
                for a in range(slabs):
                    for j in js:
                        value = x_part(cur, nxt, first + a, j, n)
                        put(first + a, j, value)
                        if not last:
                            totals[slot] = packed(value, a * lanes_of + j, totals[slot])
            if not last:
                start(("x", n), nxt)
        if not last:
            start(("y", "face"), nxt)
            for _, slot, _ in ends:
                pack[nxt][slot] = totals[slot]
            start(("z", "face"), nxt)
        wait_recv(("z", "inner"), cur)
        wait_recv(("y", "inner"), cur)

        beyond = z_beside(cur, range(2, packs))
        for m in range(inner):
            total = zero
            first = m * slabs + slabs
            for (a, j), value in yz_part(cur, nxt, first, beyond[m]).items():
                put(first + a, j, value)
                if not last:
                    total = packed(value, a * lanes_of + j, total)
            if not last:
                pack[nxt][2 + m] = total
        if not last:
            start(("z", "inner"), nxt)
            start(("y", "inner"), nxt)
    for name in every:
        wait_send(name, (STEPS - 1) % 2)


def move_out(first_ref, second_ref, first_out, second_out, sem):
    moves = [
        pltpu.make_async_copy(first_ref, first_out, sem.at[0]),
        pltpu.make_async_copy(second_ref, second_out, sem.at[1]),
    ]
    for move in moves:
        move.start()
    for move in moves:
        move.wait()


def solution(mesh):
    counts = tuple(mesh.shape[name] for name in ("gx", "gy", "gz"))

    def per_device(now, before, codes, velocity, wavelet, source_cell):
        nx, ny, nz = now.shape
        anywhere = pl.BlockSpec(memory_space=pl.ANY)
        scalars = pl.BlockSpec(memory_space=pltpu.SMEM)
        packs = nx * ny // LANES
        copies = 2 * CHUNKS + 10
        results = pl.pallas_call(
            functools.partial(kernel, (now.shape, counts)),
            out_shape=(pltpu.VMEM(now.shape, jnp.float32),) * 2,
            in_specs=[anywhere] * 3 + [scalars] * 3,
            out_specs=(pl.BlockSpec(memory_space=pltpu.VMEM),) * 2,
            scratch_shapes=[
                pltpu.VMEM((nx, ny + 2 * T, nz), jnp.float32),
                pltpu.VMEM((nx, ny + 2 * T, nz), jnp.float32),
                pltpu.VMEM((nx, ny + 2 * T, nz), jnp.float32),
                pltpu.VMEM((nx, ny + 2 * T, nz), jnp.float32),
                pltpu.VMEM((nx, ny // 8, 8, nz), jnp.float32),
                pltpu.VMEM((nx, ny // 8, 8, nz), jnp.float32),
                pltpu.VMEM((packs, 8, LANES), jnp.float32),
                pltpu.VMEM((packs, 8, LANES), jnp.float32),
                pltpu.VMEM((2, 2, CHUNKS, W, ny // 8 // CHUNKS, 8, nz), jnp.float32),
                pltpu.VMEM((nx, ny // 8, 8, nz), jnp.float32),
                pltpu.VMEM((nx, ny // 8, 8, nz), jnp.float32),
                pltpu.VMEM((nx, ny, nz), jnp.int32),
                pltpu.VMEM((nx, ny // 8, 8, nz), jnp.float32),
                pltpu.VMEM((2, 2, packs, 8, LANES), jnp.float32),
                pltpu.VMEM((nx, ny // 8, 8, nz), jnp.float32),
                pltpu.VMEM((2 * LANES, LANES), jnp.bfloat16),
                pltpu.VMEM((2 * LANES, LANES), jnp.bfloat16),
                pltpu.VMEM((8, 16, LANES), jnp.bfloat16),
                pltpu.SemaphoreType.DMA((2, copies)),
                pltpu.SemaphoreType.DMA((2, copies)),
                pltpu.SemaphoreType.DMA((3,)),
            ],
            compiler_params=pltpu.CompilerParams(collective_id=0, has_side_effects=True),
        )(now, before, codes, velocity, wavelet, source_cell)
        return pl.pallas_call(
            move_out,
            out_shape=(jax.ShapeDtypeStruct(now.shape, jnp.float32),) * 2,
            in_specs=[pl.BlockSpec(memory_space=pltpu.VMEM)] * 2,
            out_specs=(anywhere, anywhere),
            scratch_shapes=[pltpu.SemaphoreType.DMA((2,))],
            compiler_params=pltpu.CompilerParams(vmem_limit_bytes=2**20),
        )(*[pltpu.with_memory_space_constraint(value, pltpu.VMEM) for value in results])

    block = P("gx", "gy", "gz")
    return jax.shard_map(
        per_device,
        mesh=mesh,
        in_specs=(block, block, block, P(), P(), P()),
        out_specs=(block, block),
        check_vma=False,
    )
```

```python
import functools

import jax
import jax.numpy as jnp
from jax import lax
from jax.experimental import pallas as pl
from jax.experimental.pallas import tpu as pltpu
from jax.sharding import PartitionSpec as P

STEPS = 6
CENTRE = -205.0 / 72.0
C1, C2, C3, C4 = (8.0 / 5.0, -1.0 / 5.0, 8.0 / 315.0, -1.0 / 560.0)
SCALE = 5040.0
WEIGHTS = tuple(round(SCALE * c) * 1.0 for c in (C1, C2, C3, C4))
W = 4
T = 8
LANES = 128
MESH = pl.DeviceIdType.MESH
def kernel(sizes, now_hbm, before_hbm, code_hbm, vel_hbm, wave_hbm, src_hbm, out_ref, prev_ref,
           field0, field1, beside0, beside1, pack0, pack1, halo, rate, coef, code, source, edge,
           along, along_z, from_edge, only, vel_ref, wave_ref, src_ref, send_sem, recv_sem, load_sem):
    field, beside, pack = (field0, field1), (beside0, beside1), (pack0, pack1)
    (nx, ny, nz), (gx, gy, gz) = sizes
    grid_y, grid_z = ny * gy, nz * gz
    tiles = ny // 8
    fits = LANES // 8
    ix, iy, iz = lax.axis_index("gx"), lax.axis_index("gy"), lax.axis_index("gz")
    targets = (
        (({"gx": lax.rem(ix + gx - 1, gx)}, None), ({"gx": lax.rem(ix + 1, gx)}, None)),
        (({"gy": iy - 1}, iy > 0), ({"gy": iy + 1}, iy < gy - 1)),
        (({"gz": iz - 1}, iz > 0), ({"gz": iz + 1}, iz < gz - 1)),
    )

    def guarded(condition, action):
        if condition is None:
            action()
        else:
            pl.when(condition)(action)

    own_x, own_y = pl.ds(0, nx), pl.ds(T, ny)
    loads = [
        pltpu.make_async_copy(now_hbm, field[0].at[own_x, own_y], load_sem.at[0]),
        pltpu.make_async_copy(before_hbm, field[1].at[own_x, own_y], load_sem.at[1]),
        pltpu.make_async_copy(code_hbm, code, load_sem.at[2]),
        pltpu.make_async_copy(vel_hbm, vel_ref, load_sem.at[3]),
        pltpu.make_async_copy(wave_hbm, wave_ref, load_sem.at[4]),
        pltpu.make_async_copy(src_hbm, src_ref, load_sem.at[5]),
    ]
    for load in loads:
        load.start()

    for par in range(2):
        for rows in (pl.ds(0, T), pl.ds(T + ny, T)):
            beside[par][own_x, rows, :] = jnp.zeros((nx, T, LANES), jnp.float32)
    edge[...] = jnp.zeros_like(edge)

    barrier = pltpu.get_barrier_semaphore()
    for sides in targets:
        for target, present in sides:
            guarded(present, lambda target=target: pl.semaphore_signal(
                barrier, inc=1, device_id=target, device_id_type=MESH))

    nothing = jnp.zeros((nx, T, LANES), jnp.float32)
    for par in range(2):
        field[par][own_x, 0:T, :] = nothing
        field[par][own_x, pl.ds(T + ny, T), :] = nothing
        for inside in (pl.ds(T, T), pl.ds(ny, T)):
            beside[par][own_x, inside, :] = nothing

    faces = list(range(W)) + list(range(nx - W, nx))
    outer, middle = [0, tiles - 1], list(range(1, tiles - 1))
    items = [[(x, g) for x in faces for g in outer], [(x, g) for x in faces for g in middle]]
    rest = [(x, g) for x in range(W, nx - W) for g in range(tiles)]
    items += [rest[n:n + fits] for n in range(0, len(rest), fits)]
    last_slots = list(range(2, len(items)))
    spans = {"low": pl.ds(0, W), "high": pl.ds(nx - W, W), "rest": pl.ds(W, nx - 2 * W)}
    slots = {"outer": pl.ds(0, 1), "middle": pl.ds(1, 1), "rest": pl.ds(2, len(last_slots))}
    bands = {"first": (0, 1), "end": (tiles - 1, 1), "middle": (1, tiles - 2)}

    every = [("x", band, way) for band in bands for way in range(2)]
    every += [("y", part, way) for part in spans for way in range(2)]
    every += [("z", part, way) for part in slots for way in range(2)]
    x_outer = [("x", band, way) for band in ("first", "end") for way in range(2)]
    x_middle = [("x", "middle", way) for way in range(2)]
    y_outer = [("y", part, way) for way in range(2) for part in ("low", "high")]
    y_rest = [("y", "rest", way) for way in range(2)]
    z_of = {part: [("z", part, way) for way in range(2)] for part in slots}

    def transfer(name, par):
        axis, part, way = name
        if axis == "x":
            at, size = bands[part]
            layer = pl.ds(0, W) if way == 0 else pl.ds(nx - W, W)
            src = field[par].at[layer, pl.ds(T + 8 * at, 8 * size)]
            dst = halo.at[par, 1 - way, pl.ds(0, W), pl.ds(8 * at, 8 * size)]
        elif axis == "y":
            own, there = (pl.ds(T, W), pl.ds(T + ny, W)) if way == 0 else (pl.ds(T + ny - W, W), pl.ds(T - W, W))
            src, dst = field[par].at[spans[part], own], beside[par].at[spans[part], there]
        else:
            src, dst = pack[par].at[slots[part]], edge.at[par, 1 - way, slots[part]]
        sides = targets["xyz".index(axis)]
        number = every.index(name)
        copy = pltpu.make_async_remote_copy(
            src_ref=src, dst_ref=dst, send_sem=send_sem.at[par, number], recv_sem=recv_sem.at[par, number],
            device_id=sides[way][0], device_id_type=MESH)
        return copy, sides[way][1], sides[1 - way][1]

    def together(par, names, pick, action):
        groups = []
        for name in names:
            found = transfer(name, par)
            condition = found[pick]
            if groups and groups[-1][0] is condition:
                groups[-1][1].append(found[0])
            else:
                groups.append((condition, [found[0]]))
        for condition, copies in groups:
            guarded(condition, lambda copies=copies: [getattr(copy, action)() for copy in copies] and None)

    def start(par, names):
        together(par, names, 1, "start")

    def wait_sends(par):
        order = sorted(every, key=lambda name: (name[0], name[2]))
        together(par, order, 1, "wait_send")

    def wait_recv(par, names):
        together(par, names, 2, "wait_recv")

    lane = lax.broadcasted_iota(jnp.int32, (8, LANES), 1)
    group_of, place = lane // 8, lane % 8
    zero = jnp.zeros((8, LANES), jnp.float32)

    def packed(value, g, total):
        return jnp.where(group_of == g, pltpu.roll(value, (W + 8 * g) % LANES, 1), total)

    def tile(ref, x, g, shift=0):
        return ref[x, pl.ds(T + 8 * g + shift, 8), :]

    def pack_up(slot):
        total = zero
        for n, (x, g) in enumerate(items[slot]):
            total = packed(tile(field[0], x, g), n, total)
        pack[0][slot] = total

    loads[0].wait()
    for slot in range(2):
        pack_up(slot)
    peers = 2
    for sides in targets[1:]:
        for _, present in sides:
            peers = peers + present.astype(jnp.int32)
    pl.semaphore_wait(barrier, peers)
    start(0, x_outer + z_of["outer"] + y_outer + x_middle + z_of["middle"] + y_rest)
    for slot in last_slots:
        pack_up(slot)
    start(0, z_of["rest"])

    for load in loads[2:]:
        load.wait()
    squares = [vel_ref[n] * vel_ref[n] for n in range(vel_ref.shape[0])]

    def rate_slab(x, carry):
        codes = code[x]
        value = jnp.full(codes.shape, squares[0], jnp.float32)
        for n in range(1, len(squares)):
            value = jnp.where(codes == n, squares[n], value)
        rate[x] = value * (1.0 / SCALE)
        coef[x] = 2.0 + (3.0 * CENTRE) * value
        return carry

    lax.fori_loop(0, nx, rate_slab, 0)

    count = src_ref.shape[0]
    row_at = jnp.full((1, LANES), -1, jnp.int32)
    lane_row = lax.broadcasted_iota(jnp.int32, (1, LANES), 1)
    slot_col = lax.broadcasted_iota(jnp.int32, (LANES, LANES), 0)
    z_at = jnp.full((LANES, LANES), -1, jnp.int32)
    for s in range(count):
        cell = src_ref[s]
        sx = cell // (grid_y * grid_z) - ix * nx
        sy = cell // grid_z % grid_y - iy * ny
        sz = cell % grid_z - iz * nz
        here = (sx >= 0) & (sx < nx) & (sy >= 0) & (sy < ny)
        local = jnp.where(here, sx * ny + sy, -1)
        row_at = jnp.where((lane_row % count == s) & (lane_row < 3 * count), local, row_at)
        z_at = jnp.where((slot_col % count == s) & (slot_col < 3 * count), sz, z_at)
    spread = (z_at == lax.broadcasted_iota(jnp.int32, (LANES, LANES), 1)).astype(jnp.float32).astype(jnp.bfloat16)

    def source_field(t):
        wave = jnp.zeros((1, LANES), jnp.float32)
        for s in range(count):
            wave = jnp.where(lane_row % count == s, wave_ref[t, s], wave)
        high = wave.astype(jnp.bfloat16).astype(jnp.float32)
        rest = wave - high
        middle = rest.astype(jnp.bfloat16).astype(jnp.float32)
        parts = jnp.where(lane_row < count, high, jnp.where(lane_row < 2 * count, middle, rest - middle))
        slabs = LANES // ny

        def chunk(m, carry):
            row = lax.broadcasted_iota(jnp.int32, (LANES, LANES), 0) + m * LANES
            picks = jnp.where(row == row_at, parts, 0.0).astype(jnp.bfloat16)
            value = jnp.dot(picks, spread, preferred_element_type=jnp.float32)
            source[pl.ds(m * slabs, slabs)] = value.reshape(slabs, ny, LANES)
            return carry

        lax.fori_loop(0, nx // slabs, chunk, 0)

    row_in = lax.broadcasted_iota(jnp.int32, (LANES, LANES), 0)
    col_in = lax.broadcasted_iota(jnp.int32, (LANES, LANES), 1)
    spot = row_in % 8
    halo_at = jnp.where(spot < W, spot - W, LANES + spot - W)

    def taps(distance):
        value = jnp.zeros((LANES, LANES), jnp.float32)
        for k in range(1, W + 1):
            value = jnp.where((distance == k) | (distance == -k), WEIGHTS[k - 1], value)
        return value.astype(jnp.bfloat16)

    for part in range(2):
        along_z[pl.ds(part * LANES, LANES), :] = taps(row_in - col_in)
        from_edge[pl.ds(part * LANES, LANES), :] = taps(halo_at - col_in)
    double_lane = lax.broadcasted_iota(jnp.int32, (16, LANES), 1) // 8
    double_row = lax.broadcasted_iota(jnp.int32, (16, LANES), 0) // 8
    for pair in range(8):
        only[pair] = (double_lane == 2 * pair + double_row).astype(jnp.float32).astype(jnp.bfloat16)

    def split(value):
        high = value.astype(jnp.bfloat16)
        return high, (value - high.astype(jnp.float32)).astype(jnp.bfloat16)

    def z_own(cur):
        value = field[cur][own_x, own_y, :].reshape(nx * ny, LANES)
        total = jnp.dot(jnp.concatenate(split(value), axis=1), along_z[...], preferred_element_type=jnp.float32)
        along[...] = total.reshape(nx, ny, LANES)

    def z_beside(cur, chosen):
        picked = []
        for slot in chosen:
            value = jnp.where(place < W, edge[cur, 0, slot], edge[cur, 1, slot])
            high, low = split(jnp.concatenate([value, value], axis=0))
            picked += [jnp.concatenate([high * only[pair], low * only[pair]], axis=1) for pair in range(8)]
        total = jnp.dot(jnp.concatenate(picked, axis=0), from_edge[...], preferred_element_type=jnp.float32)
        return total.reshape(len(chosen), fits, 8, LANES)

    def own_part(cur, nxt):
        for x in range(nx):
            for g in range(tiles):
                at = pl.ds(8 * g, 8)
                acc = along[x, at, :]
                for k in range(1, W + 1):
                    near = tile(field[cur], x, g, k) + tile(field[cur], x, g, -k)
                    if x + k < nx:
                        near = near + tile(field[cur], x + k, g)
                    if x - k >= 0:
                        near = near + tile(field[cur], x - k, g)
                    acc = acc + WEIGHTS[k - 1] * near
                start_at = coef[x, at, :] * tile(field[cur], x, g) - tile(field[nxt], x, g)
                field[nxt][x, pl.ds(T + 8 * g, 8), :] = start_at + (rate[x, at, :] * acc + source[x, at, :])

    def y_part(cur, x, g):
        acc = None
        for k in range(1, W + 1):
            for edge_tile, shift in ((0, -k), (tiles - 1, k)):
                if g == edge_tile:
                    term = WEIGHTS[k - 1] * tile(beside[cur], x, g, shift)
                    acc = term if acc is None else acc + term
        return acc

    def x_part(cur, x, g):
        acc, at = None, pl.ds(8 * g, 8)
        for k in range(1, W + 1):
            if x - k < 0:
                term = WEIGHTS[k - 1] * halo[cur, 0, x - k + W, at, :]
            elif x + k >= nx:
                term = WEIGHTS[k - 1] * halo[cur, 1, x + k - nx, at, :]
            else:
                continue
            acc = term if acc is None else acc + term
        return acc

    loads[1].wait()
    for t in range(STEPS):
        cur, nxt = t % 2, (t + 1) % 2
        last = t == STEPS - 1

        def put(x, g, value):
            own = pl.ds(8 * g, 8)
            if last:
                out_ref[x, own, :] = value
            else:
                field[nxt][x, pl.ds(T + 8 * g, 8), :] = value
            if t == STEPS - 2:
                prev_ref[x, own, :] = value

        source_field(t)
        if t >= 1:
            wait_sends(nxt)
        z_own(cur)
        own_part(cur, nxt)
        for slot, part in enumerate(("outer", "middle")):
            wait_recv(cur, z_of[part])
            beyond = z_beside(cur, [slot])[0]
            if slot == 0:
                wait_recv(cur, y_outer)
            so_far = []
            for n, (x, g) in enumerate(items[slot]):
                acc, more = beyond[n], y_part(cur, x, g)
                so_far.append(tile(field[nxt], x, g) + rate[x, pl.ds(8 * g, 8), :] * (acc if more is None else acc + more))
            xs = x_outer if slot == 0 else x_middle
            wait_recv(cur, xs)
            total = zero
            for n, (x, g) in enumerate(items[slot]):
                value = so_far[n] + rate[x, pl.ds(8 * g, 8), :] * x_part(cur, x, g)
                put(x, g, value)
                if not last:
                    total = packed(value, n, total)
            if not last:
                start(nxt, xs)
                pack[nxt][slot] = total
                start(nxt, z_of[part] + (y_outer if slot == 0 else []))
        wait_recv(cur, z_of["rest"])
        beyond = z_beside(cur, last_slots)
        wait_recv(cur, y_rest)
        for m, slot in enumerate(last_slots):
            total = zero
            for n, (x, g) in enumerate(items[slot]):
                acc, more = beyond[m, n], y_part(cur, x, g)
                value = tile(field[nxt], x, g) + rate[x, pl.ds(8 * g, 8), :] * (acc if more is None else acc + more)
                put(x, g, value)
                if not last:
                    total = packed(value, n, total)
            if not last:
                pack[nxt][slot] = total
        if not last:
            start(nxt, z_of["rest"] + y_rest)
    wait_sends((STEPS - 1) % 2)


def move_out(first_ref, second_ref, first_out, second_out, sem):
    moves = [
        pltpu.make_async_copy(first_ref, first_out, sem.at[0]),
        pltpu.make_async_copy(second_ref, second_out, sem.at[1]),
    ]
    for move in moves:
        move.start()
    for move in moves:
        move.wait()


def solution(mesh):
    counts = tuple(mesh.shape[name] for name in ("gx", "gy", "gz"))

    def per_device(now, before, codes, velocity, wavelet, source_cell):
        nx, ny, nz = now.shape
        anywhere = pl.BlockSpec(memory_space=pl.ANY)
        packs = nx * ny // LANES
        copies = 18
        results = pl.pallas_call(
            functools.partial(kernel, (now.shape, counts)),
            out_shape=(pltpu.VMEM(now.shape, jnp.float32),) * 2,
            in_specs=[anywhere] * 6,
            out_specs=(pl.BlockSpec(memory_space=pltpu.VMEM),) * 2,
            scratch_shapes=[
                pltpu.VMEM((nx, ny + 2 * T, nz), jnp.float32),
                pltpu.VMEM((nx, ny + 2 * T, nz), jnp.float32),
                pltpu.VMEM((nx, ny + 2 * T, nz), jnp.float32),
                pltpu.VMEM((nx, ny + 2 * T, nz), jnp.float32),
                pltpu.VMEM((packs, 8, LANES), jnp.float32),
                pltpu.VMEM((packs, 8, LANES), jnp.float32),
                pltpu.VMEM((2, 2, W, ny, nz), jnp.float32),
                pltpu.VMEM((nx, ny, nz), jnp.float32),
                pltpu.VMEM((nx, ny, nz), jnp.float32),
                pltpu.VMEM((nx, ny, nz), jnp.int32),
                pltpu.VMEM((nx, ny, nz), jnp.float32),
                pltpu.VMEM((2, 2, packs, 8, LANES), jnp.float32),
                pltpu.VMEM((nx, ny, nz), jnp.float32),
                pltpu.VMEM((2 * LANES, LANES), jnp.bfloat16),
                pltpu.VMEM((2 * LANES, LANES), jnp.bfloat16),
                pltpu.VMEM((8, 16, LANES), jnp.bfloat16),
                pltpu.SMEM(velocity.shape, jnp.float32),
                pltpu.SMEM(wavelet.shape, jnp.float32),
                pltpu.SMEM(source_cell.shape, jnp.int32),
                pltpu.SemaphoreType.DMA((2, copies)),
                pltpu.SemaphoreType.DMA((2, copies)),
                pltpu.SemaphoreType.DMA((6,)),
            ],
            compiler_params=pltpu.CompilerParams(collective_id=0, has_side_effects=True),
        )(now, before, codes, velocity, wavelet, source_cell)
        return pl.pallas_call(
            move_out,
            out_shape=(jax.ShapeDtypeStruct(now.shape, jnp.float32),) * 2,
            in_specs=[pl.BlockSpec(memory_space=pltpu.VMEM)] * 2,
            out_specs=(anywhere, anywhere),
            scratch_shapes=[pltpu.SemaphoreType.DMA((2,))],
            compiler_params=pltpu.CompilerParams(vmem_limit_bytes=2**20),
        )(*[pltpu.with_memory_space_constraint(value, pltpu.VMEM) for value in results])

    block = P("gx", "gy", "gz")
    return jax.shard_map(
        per_device,
        mesh=mesh,
        in_specs=(block, block, block, P(), P(), P()),
        out_specs=(block, block),
        check_vma=False,
    )
```

```python
import functools

import jax
import jax.numpy as jnp
from jax import lax
from jax.experimental import pallas as pl
from jax.experimental.pallas import tpu as pltpu
from jax.sharding import PartitionSpec as P

STEPS = 6
CENTRE = -205.0 / 72.0
C1, C2, C3, C4 = (8.0 / 5.0, -1.0 / 5.0, 8.0 / 315.0, -1.0 / 560.0)
SCALE = 5040.0
WEIGHTS = tuple(round(SCALE * c) * 1.0 for c in (C1, C2, C3, C4))
W = 4
T = 8
LANES = 128
MESH = pl.DeviceIdType.MESH
def kernel(sizes, now_hbm, before_hbm, code_hbm, vel_hbm, wave_hbm, src_hbm, out_ref, prev_ref,
           field0, field1, beside0, beside1, pack0, pack1, halo, rate, coef, code, source, edge,
           along, along_z, from_edge, only, vel_ref, wave_ref, src_ref, send_sem, recv_sem, load_sem):
    field, beside, pack = (field0, field1), (beside0, beside1), (pack0, pack1)
    (nx, ny, nz), (gx, gy, gz) = sizes
    grid_y, grid_z = ny * gy, nz * gz
    tiles = ny // 8
    fits = LANES // 8
    ix, iy, iz = lax.axis_index("gx"), lax.axis_index("gy"), lax.axis_index("gz")
    targets = (
        (({"gx": lax.rem(ix + gx - 1, gx)}, None), ({"gx": lax.rem(ix + 1, gx)}, None)),
        (({"gy": iy - 1}, iy > 0), ({"gy": iy + 1}, iy < gy - 1)),
        (({"gz": iz - 1}, iz > 0), ({"gz": iz + 1}, iz < gz - 1)),
    )

    def guarded(condition, action):
        if condition is None:
            action()
        else:
            pl.when(condition)(action)

    own_x, own_y = pl.ds(0, nx), pl.ds(T, ny)
    loads = [
        pltpu.make_async_copy(now_hbm, field[0].at[own_x, own_y], load_sem.at[0]),
        pltpu.make_async_copy(before_hbm, field[1].at[own_x, own_y], load_sem.at[1]),
        pltpu.make_async_copy(code_hbm, code, load_sem.at[2]),
        pltpu.make_async_copy(vel_hbm, vel_ref, load_sem.at[3]),
        pltpu.make_async_copy(wave_hbm, wave_ref, load_sem.at[4]),
        pltpu.make_async_copy(src_hbm, src_ref, load_sem.at[5]),
    ]
    for load in loads:
        load.start()

    for par in range(2):
        for rows in (pl.ds(0, T), pl.ds(T + ny, T)):
            beside[par][own_x, rows, :] = jnp.zeros((nx, T, LANES), jnp.float32)
    edge[...] = jnp.zeros_like(edge)

    barrier = pltpu.get_barrier_semaphore()
    for sides in targets:
        for target, present in sides:
            guarded(present, lambda target=target: pl.semaphore_signal(
                barrier, inc=1, device_id=target, device_id_type=MESH))

    nothing = jnp.zeros((nx, T, LANES), jnp.float32)
    for par in range(2):
        field[par][own_x, 0:T, :] = nothing
        field[par][own_x, pl.ds(T + ny, T), :] = nothing
        for inside in (pl.ds(T, T), pl.ds(ny, T)):
            beside[par][own_x, inside, :] = nothing

    faces = list(range(W)) + list(range(nx - W, nx))
    outer, middle = [0, tiles - 1], list(range(1, tiles - 1))
    items = [[(x, g) for x in faces for g in outer], [(x, g) for x in faces for g in middle]]
    rest = [(x, g) for x in range(W, nx - W) for g in range(tiles)]
    items += [rest[n:n + fits] for n in range(0, len(rest), fits)]
    last_slots = list(range(2, len(items)))
    spans = {"low": pl.ds(0, W), "high": pl.ds(nx - W, W), "rest": pl.ds(W, nx - 2 * W)}
    slots = {"outer": pl.ds(0, 1), "middle": pl.ds(1, 1), "rest": pl.ds(2, len(last_slots))}
    bands = {"first": (0, 1), "end": (tiles - 1, 1), "middle": (1, tiles - 2)}

    every = [("x", band, way) for band in bands for way in range(2)]
    every += [("y", part, way) for part in spans for way in range(2)]
    every += [("z", part, way) for part in slots for way in range(2)]
    x_outer = [("x", band, way) for band in ("first", "end") for way in range(2)]
    x_middle = [("x", "middle", way) for way in range(2)]
    y_outer = [("y", part, way) for way in range(2) for part in ("low", "high")]
    y_rest = [("y", "rest", way) for way in range(2)]
    z_of = {part: [("z", part, way) for way in range(2)] for part in slots}

    def transfer(name, par):
        axis, part, way = name
        if axis == "x":
            at, size = bands[part]
            layer = pl.ds(0, W) if way == 0 else pl.ds(nx - W, W)
            src = field[par].at[layer, pl.ds(T + 8 * at, 8 * size)]
            dst = halo.at[par, 1 - way, pl.ds(0, W), pl.ds(8 * at, 8 * size)]
        elif axis == "y":
            own, there = (pl.ds(T, W), pl.ds(T + ny, W)) if way == 0 else (pl.ds(T + ny - W, W), pl.ds(T - W, W))
            src, dst = field[par].at[spans[part], own], beside[par].at[spans[part], there]
        else:
            src, dst = pack[par].at[slots[part]], edge.at[par, 1 - way, slots[part]]
        sides = targets["xyz".index(axis)]
        number = every.index(name)
        copy = pltpu.make_async_remote_copy(
            src_ref=src, dst_ref=dst, send_sem=send_sem.at[par, number], recv_sem=recv_sem.at[par, number],
            device_id=sides[way][0], device_id_type=MESH)
        return copy, sides[way][1], sides[1 - way][1]

    def together(par, names, pick, action):
        groups = []
        for name in names:
            found = transfer(name, par)
            condition = found[pick]
            if groups and groups[-1][0] is condition:
                groups[-1][1].append(found[0])
            else:
                groups.append((condition, [found[0]]))
        for condition, copies in groups:
            guarded(condition, lambda copies=copies: [getattr(copy, action)() for copy in copies] and None)

    def start(par, names):
        together(par, names, 1, "start")

    def wait_sends(par):
        order = sorted(every, key=lambda name: (name[0], name[2]))
        together(par, order, 1, "wait_send")

    def wait_recv(par, names):
        together(par, names, 2, "wait_recv")

    lane = lax.broadcasted_iota(jnp.int32, (8, LANES), 1)
    group_of, place = lane // 8, lane % 8
    zero = jnp.zeros((8, LANES), jnp.float32)

    def packed(value, g, total):
        return jnp.where(group_of == g, pltpu.roll(value, (W + 8 * g) % LANES, 1), total)

    def tile(ref, x, g, shift=0):
        return ref[x, pl.ds(T + 8 * g + shift, 8), :]

    def pack_up(slot):
        total = zero
        for n, (x, g) in enumerate(items[slot]):
            total = packed(tile(field[0], x, g), n, total)
        pack[0][slot] = total

    loads[0].wait()
    for slot in range(2):
        pack_up(slot)
    peers = 2
    for sides in targets[1:]:
        for _, present in sides:
            peers = peers + present.astype(jnp.int32)
    pl.semaphore_wait(barrier, peers)
    start(0, x_outer + z_of["outer"] + y_outer + x_middle + z_of["middle"] + y_rest)
    for slot in last_slots:
        pack_up(slot)
    start(0, z_of["rest"])

    for load in loads[2:]:
        load.wait()
    squares = [vel_ref[n] * vel_ref[n] for n in range(vel_ref.shape[0])]

    def rate_slab(x, carry):
        codes = code[x]
        value = jnp.full(codes.shape, squares[0], jnp.float32)
        for n in range(1, len(squares)):
            value = jnp.where(codes == n, squares[n], value)
        rate[x] = value * (1.0 / SCALE)
        coef[x] = 2.0 + (3.0 * CENTRE) * value
        return carry

    lax.fori_loop(0, nx, rate_slab, 0)

    count = src_ref.shape[0]
    row_at = jnp.full((1, LANES), -1, jnp.int32)
    lane_row = lax.broadcasted_iota(jnp.int32, (1, LANES), 1)
    slot_col = lax.broadcasted_iota(jnp.int32, (LANES, LANES), 0)
    z_at = jnp.full((LANES, LANES), -1, jnp.int32)
    for s in range(count):
        cell = src_ref[s]
        sx = cell // (grid_y * grid_z) - ix * nx
        sy = cell // grid_z % grid_y - iy * ny
        sz = cell % grid_z - iz * nz
        here = (sx >= 0) & (sx < nx) & (sy >= 0) & (sy < ny)
        local = jnp.where(here, sx * ny + sy, -1)
        row_at = jnp.where((lane_row % count == s) & (lane_row < 3 * count), local, row_at)
        z_at = jnp.where((slot_col % count == s) & (slot_col < 3 * count), sz, z_at)
    spread = (z_at == lax.broadcasted_iota(jnp.int32, (LANES, LANES), 1)).astype(jnp.float32).astype(jnp.bfloat16)

    def source_field(t):
        wave = jnp.zeros((1, LANES), jnp.float32)
        for s in range(count):
            wave = jnp.where(lane_row % count == s, wave_ref[t, s], wave)
        high = wave.astype(jnp.bfloat16).astype(jnp.float32)
        rest = wave - high
        middle = rest.astype(jnp.bfloat16).astype(jnp.float32)
        parts = jnp.where(lane_row < count, high, jnp.where(lane_row < 2 * count, middle, rest - middle))
        slabs = LANES // ny

        def chunk(m, carry):
            row = lax.broadcasted_iota(jnp.int32, (LANES, LANES), 0) + m * LANES
            picks = jnp.where(row == row_at, parts, 0.0).astype(jnp.bfloat16)
            value = jnp.dot(picks, spread, preferred_element_type=jnp.float32)
            source[pl.ds(m * slabs, slabs)] = value.reshape(slabs, ny, LANES)
            return carry

        lax.fori_loop(0, nx // slabs, chunk, 0)

    row_in = lax.broadcasted_iota(jnp.int32, (LANES, LANES), 0)
    col_in = lax.broadcasted_iota(jnp.int32, (LANES, LANES), 1)
    spot = row_in % 8
    halo_at = jnp.where(spot < W, spot - W, LANES + spot - W)

    def taps(distance):
        value = jnp.zeros((LANES, LANES), jnp.float32)
        for k in range(1, W + 1):
            value = jnp.where((distance == k) | (distance == -k), WEIGHTS[k - 1], value)
        return value.astype(jnp.bfloat16)

    for part in range(2):
        along_z[pl.ds(part * LANES, LANES), :] = taps(row_in - col_in)
        from_edge[pl.ds(part * LANES, LANES), :] = taps(halo_at - col_in)
    double_lane = lax.broadcasted_iota(jnp.int32, (16, LANES), 1) // 8
    double_row = lax.broadcasted_iota(jnp.int32, (16, LANES), 0) // 8
    for pair in range(8):
        only[pair] = (double_lane == 2 * pair + double_row).astype(jnp.float32).astype(jnp.bfloat16)

    def split(value):
        high = value.astype(jnp.bfloat16)
        return high, (value - high.astype(jnp.float32)).astype(jnp.bfloat16)

    def z_own(cur):
        value = field[cur][own_x, own_y, :].reshape(nx * ny, LANES)
        total = jnp.dot(jnp.concatenate(split(value), axis=1), along_z[...], preferred_element_type=jnp.float32)
        along[...] = total.reshape(nx, ny, LANES)

    def z_beside(cur, chosen):
        picked = []
        for slot in chosen:
            value = jnp.where(place < W, edge[cur, 0, slot], edge[cur, 1, slot])
            high, low = split(jnp.concatenate([value, value], axis=0))
            picked += [jnp.concatenate([high * only[pair], low * only[pair]], axis=1) for pair in range(8)]
        total = jnp.dot(jnp.concatenate(picked, axis=0), from_edge[...], preferred_element_type=jnp.float32)
        return total.reshape(len(chosen), fits, 8, LANES)

    def own_part(cur, nxt):
        for x in range(nx):
            for g in range(tiles):
                at = pl.ds(8 * g, 8)
                acc = along[x, at, :]
                for k in range(1, W + 1):
                    near = tile(field[cur], x, g, k) + tile(field[cur], x, g, -k)
                    if x + k < nx:
                        near = near + tile(field[cur], x + k, g)
                    if x - k >= 0:
                        near = near + tile(field[cur], x - k, g)
                    acc = acc + WEIGHTS[k - 1] * near
                start_at = coef[x, at, :] * tile(field[cur], x, g) - tile(field[nxt], x, g)
                field[nxt][x, pl.ds(T + 8 * g, 8), :] = start_at + (rate[x, at, :] * acc + source[x, at, :])

    def y_part(cur, x, g):
        acc = None
        for k in range(1, W + 1):
            for edge_tile, shift in ((0, -k), (tiles - 1, k)):
                if g == edge_tile:
                    term = WEIGHTS[k - 1] * tile(beside[cur], x, g, shift)
                    acc = term if acc is None else acc + term
        return acc

    def x_part(cur, x, g):
        acc, at = None, pl.ds(8 * g, 8)
        for k in range(1, W + 1):
            if x - k < 0:
                term = WEIGHTS[k - 1] * halo[cur, 0, x - k + W, at, :]
            elif x + k >= nx:
                term = WEIGHTS[k - 1] * halo[cur, 1, x + k - nx, at, :]
            else:
                continue
            acc = term if acc is None else acc + term
        return acc

    loads[1].wait()
    for t in range(STEPS):
        cur, nxt = t % 2, (t + 1) % 2
        last = t == STEPS - 1

        def put(x, g, value):
            own = pl.ds(8 * g, 8)
            if last:
                out_ref[x, own, :] = value
            else:
                field[nxt][x, pl.ds(T + 8 * g, 8), :] = value
            if t == STEPS - 2:
                prev_ref[x, own, :] = value

        source_field(t)
        if t >= 1:
            wait_sends(nxt)
        z_own(cur)
        own_part(cur, nxt)
        for slot, part in enumerate(("outer", "middle")):
            wait_recv(cur, z_of[part])
            beyond = z_beside(cur, [slot])[0]
            if slot == 0:
                wait_recv(cur, y_outer)
            so_far = []
            for n, (x, g) in enumerate(items[slot]):
                acc, more = beyond[n], y_part(cur, x, g)
                so_far.append(tile(field[nxt], x, g) + rate[x, pl.ds(8 * g, 8), :] * (acc if more is None else acc + more))
            xs = x_outer if slot == 0 else x_middle
            wait_recv(cur, xs)
            total = zero
            for n, (x, g) in enumerate(items[slot]):
                value = so_far[n] + rate[x, pl.ds(8 * g, 8), :] * x_part(cur, x, g)
                put(x, g, value)
                if not last:
                    total = packed(value, n, total)
            if not last:
                start(nxt, xs)
                pack[nxt][slot] = total
                start(nxt, z_of[part] + (y_outer if slot == 0 else []))
        wait_recv(cur, z_of["rest"])
        beyond = z_beside(cur, last_slots)
        wait_recv(cur, y_rest)
        for m, slot in enumerate(last_slots):
            total = zero
            for n, (x, g) in enumerate(items[slot]):
                acc, more = beyond[m, n], y_part(cur, x, g)
                value = tile(field[nxt], x, g) + rate[x, pl.ds(8 * g, 8), :] * (acc if more is None else acc + more)
                put(x, g, value)
                if not last:
                    total = packed(value, n, total)
            if not last:
                pack[nxt][slot] = total
        if not last:
            start(nxt, z_of["rest"] + y_rest)
    wait_sends((STEPS - 1) % 2)


def scoped(sizes, *refs):
    copies = 18
    pl.run_scoped(
        functools.partial(kernel, sizes, *refs),
        pltpu.SemaphoreType.DMA((2, copies)),
        pltpu.SemaphoreType.DMA((2, copies)),
        pltpu.SemaphoreType.DMA((6,)),
    )


def move_out(first_ref, second_ref, first_out, second_out, sem):
    moves = [
        pltpu.make_async_copy(first_ref, first_out, sem.at[0]),
        pltpu.make_async_copy(second_ref, second_out, sem.at[1]),
    ]
    for move in moves:
        move.start()
    for move in moves:
        move.wait()


def solution(mesh):
    counts = tuple(mesh.shape[name] for name in ("gx", "gy", "gz"))

    def per_device(now, before, codes, velocity, wavelet, source_cell):
        nx, ny, nz = now.shape
        anywhere = pl.BlockSpec(memory_space=pl.ANY)
        packs = nx * ny // LANES
        results = pl.pallas_call(
            functools.partial(scoped, (now.shape, counts)),
            out_shape=(pltpu.VMEM(now.shape, jnp.float32),) * 2,
            in_specs=[anywhere] * 6,
            out_specs=(pl.BlockSpec(memory_space=pltpu.VMEM),) * 2,
            scratch_shapes=[
                pltpu.VMEM((nx, ny + 2 * T, nz), jnp.float32),
                pltpu.VMEM((nx, ny + 2 * T, nz), jnp.float32),
                pltpu.VMEM((nx, ny + 2 * T, nz), jnp.float32),
                pltpu.VMEM((nx, ny + 2 * T, nz), jnp.float32),
                pltpu.VMEM((packs, 8, LANES), jnp.float32),
                pltpu.VMEM((packs, 8, LANES), jnp.float32),
                pltpu.VMEM((2, 2, W, ny, nz), jnp.float32),
                pltpu.VMEM((nx, ny, nz), jnp.float32),
                pltpu.VMEM((nx, ny, nz), jnp.float32),
                pltpu.VMEM((nx, ny, nz), jnp.int32),
                pltpu.VMEM((nx, ny, nz), jnp.float32),
                pltpu.VMEM((2, 2, packs, 8, LANES), jnp.float32),
                pltpu.VMEM((nx, ny, nz), jnp.float32),
                pltpu.VMEM((2 * LANES, LANES), jnp.bfloat16),
                pltpu.VMEM((2 * LANES, LANES), jnp.bfloat16),
                pltpu.VMEM((8, 16, LANES), jnp.bfloat16),
                pltpu.SMEM(velocity.shape, jnp.float32),
                pltpu.SMEM(wavelet.shape, jnp.float32),
                pltpu.SMEM(source_cell.shape, jnp.int32),
            ],
            compiler_params=pltpu.CompilerParams(collective_id=0, has_side_effects=True),
        )(now, before, codes, velocity, wavelet, source_cell)
        return pl.pallas_call(
            move_out,
            out_shape=(jax.ShapeDtypeStruct(now.shape, jnp.float32),) * 2,
            in_specs=[pl.BlockSpec(memory_space=pltpu.VMEM)] * 2,
            out_specs=(anywhere, anywhere),
            scratch_shapes=[pltpu.SemaphoreType.DMA((2,))],
            compiler_params=pltpu.CompilerParams(vmem_limit_bytes=2**20),
        )(*[pltpu.with_memory_space_constraint(value, pltpu.VMEM) for value in results])

    block = P("gx", "gy", "gz")
    return jax.shard_map(
        per_device,
        mesh=mesh,
        in_specs=(block, block, block, P(), P(), P()),
        out_specs=(block, block),
        check_vma=False,
    )
```

```python
import functools

import jax
import jax.numpy as jnp
from jax import lax
from jax.experimental import pallas as pl
from jax.experimental.pallas import tpu as pltpu
from jax.sharding import PartitionSpec as P

STEPS = 6
CENTRE = -205.0 / 72.0
C1, C2, C3, C4 = (8.0 / 5.0, -1.0 / 5.0, 8.0 / 315.0, -1.0 / 560.0)
SCALE = 5040.0
WEIGHTS = tuple(round(SCALE * c) * 1.0 for c in (C1, C2, C3, C4))
W = 4
T = 8
LANES = 128
MESH = pl.DeviceIdType.MESH
def kernel(sizes, now_hbm, before_hbm, code_hbm, vel_hbm, wave_hbm, src_hbm, out_ref, prev_ref,
           field0, field1, beside0, beside1, pack0, pack1, halo, rate, coef, code, source, edge,
           along, along_z, from_edge, only, vel_ref, wave_ref, src_ref, send_sem, recv_sem, load_sem):
    field, beside, pack = (field0, field1), (beside0, beside1), (pack0, pack1)
    (nx, ny, nz), (gx, gy, gz) = sizes
    grid_y, grid_z = ny * gy, nz * gz
    tiles = ny // 8
    fits = LANES // 8
    ix, iy, iz = lax.axis_index("gx"), lax.axis_index("gy"), lax.axis_index("gz")
    targets = (
        (({"gx": lax.rem(ix + gx - 1, gx)}, None), ({"gx": lax.rem(ix + 1, gx)}, None)),
        (({"gy": iy - 1}, iy > 0), ({"gy": iy + 1}, iy < gy - 1)),
        (({"gz": iz - 1}, iz > 0), ({"gz": iz + 1}, iz < gz - 1)),
    )

    def guarded(condition, action):
        if condition is None:
            action()
        else:
            pl.when(condition)(action)

    own_x, own_y = pl.ds(0, nx), pl.ds(T, ny)
    loads = [
        pltpu.make_async_copy(now_hbm, field[0].at[own_x, own_y], load_sem.at[0]),
        pltpu.make_async_copy(before_hbm, field[1].at[own_x, own_y], load_sem.at[1]),
        pltpu.make_async_copy(code_hbm, code, load_sem.at[2]),
        pltpu.make_async_copy(vel_hbm, vel_ref, load_sem.at[3]),
        pltpu.make_async_copy(wave_hbm, wave_ref, load_sem.at[4]),
        pltpu.make_async_copy(src_hbm, src_ref, load_sem.at[5]),
    ]
    for load in loads:
        load.start()

    barrier = pltpu.get_barrier_semaphore()
    for sides in targets:
        for target, present in sides:
            guarded(present, lambda target=target: pl.semaphore_signal(
                barrier, inc=1, device_id=target, device_id_type=MESH))

    nothing = jnp.zeros((nx, T, LANES), jnp.float32)

    def clear(way):
        def rows():
            for par in range(2):
                beside[par][own_x, pl.ds(way * (T + ny), T), :] = nothing

        def packs():
            for par in range(2):
                edge[par, way] = jnp.zeros(edge.shape[2:], jnp.float32)

        pl.when(jnp.logical_not(targets[1][way][1]))(rows)
        pl.when(jnp.logical_not(targets[2][way][1]))(packs)

    clear(0)
    clear(1)
    for par in range(2):
        field[par][own_x, 0:T, :] = nothing
        field[par][own_x, pl.ds(T + ny, T), :] = nothing
        for inside in (pl.ds(T, T), pl.ds(ny, T)):
            beside[par][own_x, inside, :] = nothing

    faces = list(range(W)) + list(range(nx - W, nx))
    outer, middle = [0, tiles - 1], list(range(1, tiles - 1))
    items = [[(x, g) for x in faces for g in outer], [(x, g) for x in faces for g in middle]]
    rest = [(x, g) for x in range(W, nx - W) for g in range(tiles)]
    items += [rest[n:n + fits] for n in range(0, len(rest), fits)]
    last_slots = list(range(2, len(items)))
    spans = {"low": pl.ds(0, W), "high": pl.ds(nx - W, W), "rest": pl.ds(W, nx - 2 * W)}
    slots = {"outer": pl.ds(0, 1), "middle": pl.ds(1, 1), "rest": pl.ds(2, len(last_slots))}
    bands = {"first": (0, 1), "end": (tiles - 1, 1), "middle": (1, tiles - 2)}

    every = [("x", band, way) for band in bands for way in range(2)]
    every += [("y", part, way) for part in spans for way in range(2)]
    every += [("z", part, way) for part in slots for way in range(2)]
    x_outer = [("x", band, way) for band in ("first", "end") for way in range(2)]
    x_middle = [("x", "middle", way) for way in range(2)]
    y_outer = [("y", part, way) for way in range(2) for part in ("low", "high")]
    y_rest = [("y", "rest", way) for way in range(2)]
    z_of = {part: [("z", part, way) for way in range(2)] for part in slots}

    def transfer(name, par):
        axis, part, way = name
        if axis == "x":
            at, size = bands[part]
            layer = pl.ds(0, W) if way == 0 else pl.ds(nx - W, W)
            src = field[par].at[layer, pl.ds(T + 8 * at, 8 * size)]
            dst = halo.at[par, 1 - way, pl.ds(0, W), pl.ds(8 * at, 8 * size)]
        elif axis == "y":
            own, there = (pl.ds(T, W), pl.ds(T + ny, W)) if way == 0 else (pl.ds(T + ny - W, W), pl.ds(T - W, W))
            src, dst = field[par].at[spans[part], own], beside[par].at[spans[part], there]
        else:
            src, dst = pack[par].at[slots[part]], edge.at[par, 1 - way, slots[part]]
        sides = targets["xyz".index(axis)]
        number = every.index(name)
        copy = pltpu.make_async_remote_copy(
            src_ref=src, dst_ref=dst, send_sem=send_sem.at[par, number], recv_sem=recv_sem.at[par, number],
            device_id=sides[way][0], device_id_type=MESH)
        return copy, sides[way][1], sides[1 - way][1]

    def together(par, names, pick, action):
        groups = []
        for name in names:
            found = transfer(name, par)
            condition = found[pick]
            if groups and groups[-1][0] is condition:
                groups[-1][1].append(found[0])
            else:
                groups.append((condition, [found[0]]))
        for condition, copies in groups:
            guarded(condition, lambda copies=copies: [getattr(copy, action)() for copy in copies] and None)

    def start(par, names):
        together(par, names, 1, "start")

    def wait_sends(par):
        order = sorted(every, key=lambda name: (name[0], name[2]))
        together(par, order, 1, "wait_send")

    def wait_recv(par, names):
        together(par, names, 2, "wait_recv")

    lane = lax.broadcasted_iota(jnp.int32, (8, LANES), 1)
    group_of, place = lane // 8, lane % 8
    zero = jnp.zeros((8, LANES), jnp.float32)

    def packed(value, g, total):
        return jnp.where(group_of == g, pltpu.roll(value, (W + 8 * g) % LANES, 1), total)

    def tile(ref, x, g, shift=0):
        return ref[x, pl.ds(T + 8 * g + shift, 8), :]

    def pack_up(slot):
        total = zero
        for n, (x, g) in enumerate(items[slot]):
            total = packed(tile(field[0], x, g), n, total)
        pack[0][slot] = total

    loads[0].wait()
    peers = 2
    for sides in targets[1:]:
        for _, present in sides:
            peers = peers + present.astype(jnp.int32)
    pl.semaphore_wait(barrier, peers)
    start(0, x_outer)
    pack_up(0)
    start(0, z_of["outer"] + y_outer + x_middle)
    pack_up(1)
    start(0, z_of["middle"] + y_rest)
    for slot in last_slots:
        pack_up(slot)
    start(0, z_of["rest"])

    for load in loads[2:]:
        load.wait()
    squares = [vel_ref[n] * vel_ref[n] for n in range(vel_ref.shape[0])]

    def rate_slab(x, carry):
        codes = code[x]
        value = jnp.full(codes.shape, squares[0], jnp.float32)
        for n in range(1, len(squares)):
            value = jnp.where(codes == n, squares[n], value)
        rate[x] = value * (1.0 / SCALE)
        coef[x] = 2.0 + (3.0 * CENTRE) * value
        return carry

    lax.fori_loop(0, nx, rate_slab, 0)

    count = src_ref.shape[0]
    row_at = jnp.full((1, LANES), -1, jnp.int32)
    lane_row = lax.broadcasted_iota(jnp.int32, (1, LANES), 1)
    slot_col = lax.broadcasted_iota(jnp.int32, (LANES, LANES), 0)
    z_at = jnp.full((LANES, LANES), -1, jnp.int32)
    for s in range(count):
        cell = src_ref[s]
        sx = cell // (grid_y * grid_z) - ix * nx
        sy = cell // grid_z % grid_y - iy * ny
        sz = cell % grid_z - iz * nz
        here = (sx >= 0) & (sx < nx) & (sy >= 0) & (sy < ny)
        local = jnp.where(here, sx * ny + sy, -1)
        row_at = jnp.where((lane_row % count == s) & (lane_row < 3 * count), local, row_at)
        z_at = jnp.where((slot_col % count == s) & (slot_col < 3 * count), sz, z_at)
    spread = (z_at == lax.broadcasted_iota(jnp.int32, (LANES, LANES), 1)).astype(jnp.float32).astype(jnp.bfloat16)

    def source_field(t):
        wave = jnp.zeros((1, LANES), jnp.float32)
        for s in range(count):
            wave = jnp.where(lane_row % count == s, wave_ref[t, s], wave)
        high = wave.astype(jnp.bfloat16).astype(jnp.float32)
        rest = wave - high
        middle = rest.astype(jnp.bfloat16).astype(jnp.float32)
        parts = jnp.where(lane_row < count, high, jnp.where(lane_row < 2 * count, middle, rest - middle))
        slabs = LANES // ny

        def chunk(m, carry):
            row = lax.broadcasted_iota(jnp.int32, (LANES, LANES), 0) + m * LANES
            picks = jnp.where(row == row_at, parts, 0.0).astype(jnp.bfloat16)
            value = jnp.dot(picks, spread, preferred_element_type=jnp.float32)
            source[pl.ds(m * slabs, slabs)] = value.reshape(slabs, ny, LANES)
            return carry

        lax.fori_loop(0, nx // slabs, chunk, 0)

    row_in = lax.broadcasted_iota(jnp.int32, (LANES, LANES), 0)
    col_in = lax.broadcasted_iota(jnp.int32, (LANES, LANES), 1)
    spot = row_in % 8
    halo_at = jnp.where(spot < W, spot - W, LANES + spot - W)

    def taps(distance):
        value = jnp.zeros((LANES, LANES), jnp.float32)
        for k in range(1, W + 1):
            value = jnp.where((distance == k) | (distance == -k), WEIGHTS[k - 1], value)
        return value.astype(jnp.bfloat16)

    for part in range(2):
        along_z[pl.ds(part * LANES, LANES), :] = taps(row_in - col_in)
        from_edge[pl.ds(part * LANES, LANES), :] = taps(halo_at - col_in)
    double_lane = lax.broadcasted_iota(jnp.int32, (16, LANES), 1) // 8
    double_row = lax.broadcasted_iota(jnp.int32, (16, LANES), 0) // 8
    for pair in range(8):
        only[pair] = (double_lane == 2 * pair + double_row).astype(jnp.float32).astype(jnp.bfloat16)

    def split(value):
        high = value.astype(jnp.bfloat16)
        return high, (value - high.astype(jnp.float32)).astype(jnp.bfloat16)

    def z_own(cur):
        value = field[cur][own_x, own_y, :].reshape(nx * ny, LANES)
        total = jnp.dot(jnp.concatenate(split(value), axis=1), along_z[...], preferred_element_type=jnp.float32)
        along[...] = total.reshape(nx, ny, LANES)

    def z_beside(cur, chosen):
        picked = []
        for slot in chosen:
            value = jnp.where(place < W, edge[cur, 0, slot], edge[cur, 1, slot])
            high, low = split(jnp.concatenate([value, value], axis=0))
            picked += [high * only[pair] for pair in range(8)] + [low * only[pair] for pair in range(8)]
        total = jnp.dot(jnp.concatenate(picked, axis=0), from_edge[0:LANES, :], preferred_element_type=jnp.float32)
        total = total.reshape(len(chosen), 2, fits, 8, LANES)
        return total[:, 0] + total[:, 1]

    def own_part(cur, nxt):
        for x in range(nx):
            for g in range(tiles):
                at = pl.ds(8 * g, 8)
                acc = along[x, at, :]
                for k in range(1, W + 1):
                    near = tile(field[cur], x, g, k) + tile(field[cur], x, g, -k)
                    if x + k < nx:
                        near = near + tile(field[cur], x + k, g)
                    if x - k >= 0:
                        near = near + tile(field[cur], x - k, g)
                    acc = acc + WEIGHTS[k - 1] * near
                start_at = coef[x, at, :] * tile(field[cur], x, g) - tile(field[nxt], x, g)
                field[nxt][x, pl.ds(T + 8 * g, 8), :] = start_at + (rate[x, at, :] * acc + source[x, at, :])

    def y_part(cur, x, g):
        acc = None
        for k in range(1, W + 1):
            for edge_tile, shift in ((0, -k), (tiles - 1, k)):
                if g == edge_tile:
                    term = WEIGHTS[k - 1] * tile(beside[cur], x, g, shift)
                    acc = term if acc is None else acc + term
        return acc

    def x_part(cur, x, g):
        acc, at = None, pl.ds(8 * g, 8)
        for k in range(1, W + 1):
            if x - k < 0:
                term = WEIGHTS[k - 1] * halo[cur, 0, x - k + W, at, :]
            elif x + k >= nx:
                term = WEIGHTS[k - 1] * halo[cur, 1, x + k - nx, at, :]
            else:
                continue
            acc = term if acc is None else acc + term
        return acc

    loads[1].wait()
    for t in range(STEPS):
        cur, nxt = t % 2, (t + 1) % 2
        last = t == STEPS - 1

        def put(x, g, value):
            own = pl.ds(8 * g, 8)
            if last:
                out_ref[x, own, :] = value
            else:
                field[nxt][x, pl.ds(T + 8 * g, 8), :] = value
            if t == STEPS - 2:
                prev_ref[x, own, :] = value

        source_field(t)
        if t >= 1:
            wait_sends(nxt)
        z_own(cur)
        own_part(cur, nxt)
        for slot, part in enumerate(("outer", "middle")):
            wait_recv(cur, z_of[part])
            beyond = z_beside(cur, [slot])[0]
            if slot == 0:
                wait_recv(cur, y_outer)
            so_far = []
            for n, (x, g) in enumerate(items[slot]):
                acc, more = beyond[n], y_part(cur, x, g)
                so_far.append(tile(field[nxt], x, g) + rate[x, pl.ds(8 * g, 8), :] * (acc if more is None else acc + more))
            xs = x_outer if slot == 0 else x_middle
            wait_recv(cur, xs)
            total = zero
            for n, (x, g) in enumerate(items[slot]):
                value = so_far[n] + rate[x, pl.ds(8 * g, 8), :] * x_part(cur, x, g)
                put(x, g, value)
                if not last:
                    total = packed(value, n, total)
            if not last:
                start(nxt, xs)
                pack[nxt][slot] = total
                start(nxt, z_of[part] + (y_outer if slot == 0 else []))
        wait_recv(cur, z_of["rest"])
        beyond = z_beside(cur, last_slots)
        wait_recv(cur, y_rest)
        for m, slot in enumerate(last_slots):
            total = zero
            for n, (x, g) in enumerate(items[slot]):
                acc, more = beyond[m, n], y_part(cur, x, g)
                value = tile(field[nxt], x, g) + rate[x, pl.ds(8 * g, 8), :] * (acc if more is None else acc + more)
                put(x, g, value)
                if not last:
                    total = packed(value, n, total)
            if not last:
                pack[nxt][slot] = total
        if not last:
            start(nxt, z_of["rest"] + y_rest)
    wait_sends((STEPS - 1) % 2)


def scoped(sizes, *refs):
    copies = 18
    pl.run_scoped(
        functools.partial(kernel, sizes, *refs),
        pltpu.SemaphoreType.DMA((2, copies)),
        pltpu.SemaphoreType.DMA((2, copies)),
        pltpu.SemaphoreType.DMA((6,)),
    )


def move_out(first_ref, second_ref, first_out, second_out, sem):
    moves = [
        pltpu.make_async_copy(first_ref, first_out, sem.at[0]),
        pltpu.make_async_copy(second_ref, second_out, sem.at[1]),
    ]
    for move in moves:
        move.start()
    for move in moves:
        move.wait()


def solution(mesh):
    counts = tuple(mesh.shape[name] for name in ("gx", "gy", "gz"))

    def per_device(now, before, codes, velocity, wavelet, source_cell):
        nx, ny, nz = now.shape
        anywhere = pl.BlockSpec(memory_space=pl.ANY)
        packs = nx * ny // LANES
        results = pl.pallas_call(
            functools.partial(scoped, (now.shape, counts)),
            out_shape=(pltpu.VMEM(now.shape, jnp.float32),) * 2,
            in_specs=[anywhere] * 6,
            out_specs=(pl.BlockSpec(memory_space=pltpu.VMEM),) * 2,
            scratch_shapes=[
                pltpu.VMEM((nx, ny + 2 * T, nz), jnp.float32),
                pltpu.VMEM((nx, ny + 2 * T, nz), jnp.float32),
                pltpu.VMEM((nx, ny + 2 * T, nz), jnp.float32),
                pltpu.VMEM((nx, ny + 2 * T, nz), jnp.float32),
                pltpu.VMEM((packs, 8, LANES), jnp.float32),
                pltpu.VMEM((packs, 8, LANES), jnp.float32),
                pltpu.VMEM((2, 2, W, ny, nz), jnp.float32),
                pltpu.VMEM((nx, ny, nz), jnp.float32),
                pltpu.VMEM((nx, ny, nz), jnp.float32),
                pltpu.VMEM((nx, ny, nz), jnp.int32),
                pltpu.VMEM((nx, ny, nz), jnp.float32),
                pltpu.VMEM((2, 2, packs, 8, LANES), jnp.float32),
                pltpu.VMEM((nx, ny, nz), jnp.float32),
                pltpu.VMEM((2 * LANES, LANES), jnp.bfloat16),
                pltpu.VMEM((2 * LANES, LANES), jnp.bfloat16),
                pltpu.VMEM((8, 16, LANES), jnp.bfloat16),
                pltpu.SMEM(velocity.shape, jnp.float32),
                pltpu.SMEM(wavelet.shape, jnp.float32),
                pltpu.SMEM(source_cell.shape, jnp.int32),
            ],
            compiler_params=pltpu.CompilerParams(collective_id=0, has_side_effects=True),
        )(now, before, codes, velocity, wavelet, source_cell)
        return pl.pallas_call(
            move_out,
            out_shape=(jax.ShapeDtypeStruct(now.shape, jnp.float32),) * 2,
            in_specs=[pl.BlockSpec(memory_space=pltpu.VMEM)] * 2,
            out_specs=(anywhere, anywhere),
            scratch_shapes=[pltpu.SemaphoreType.DMA((2,))],
            compiler_params=pltpu.CompilerParams(vmem_limit_bytes=2**20),
        )(*[pltpu.with_memory_space_constraint(value, pltpu.VMEM) for value in results])

    block = P("gx", "gy", "gz")
    return jax.shard_map(
        per_device,
        mesh=mesh,
        in_specs=(block, block, block, P(), P(), P()),
        out_specs=(block, block),
        check_vma=False,
    )
```
